64 devices in a mesh: dp: 4 (over x, y), ep: 16 (over z, core).
Axes of the slice: x: 2, y: 2, z: 8, core: 2. Of those that a mesh axis runs over, the one named last changes fastest.
The devices are a block of a 4x4x8 slice.
Arguments:
- tokens: bfloat16 [32768, 2048], P(('dp', 'ep')), parts along dimension 0
- w_router: bfloat16 [2048, 64], replicated
- expert_ids: int32 [32768, 6], P(('dp', 'ep')), parts along dimension 0
- w_gate: bfloat16 [64, 2048, 1408], P('ep')
- w_up: bfloat16 [64, 2048, 1408], P('ep')
- w_down: bfloat16 [64, 1408, 2048], P('ep')
- shared_gate: bfloat16 [2048, 2816], replicated
- shared_up: bfloat16 [2048, 2816], replicated
- shared_down: bfloat16 [2816, 2048], replicated
Outputs:
- output: bfloat16 [32768, 2048], P(('dp', 'ep')), parts along dimension 0
There are 4 independent parts. The reference program is written for one: setup_inputs(seed, part) draws one part's arguments, and reference() takes and returns one part's arrays. A program takes and returns all parts, laid end to end along the dimension named above; an argument that names none is the same for every part.
All inputs are finite; a program needn't handle non-finite values.
Results may differ from the reference program's by a relative error of at most 0.00812751.
Values are sent between devices in bfloat16 or wider.
A program may use at most 768 MiB of HBM per device.

```python
import jax
import jax.numpy as jnp
from jax import lax

MODEL_DIM = 2048
EXPERT_FF = 1408
SHARED_FF = 2816
NUM_EXPERTS = 64
TOP_K = 6
TOKENS_DEV = 512
GROUP_SIZE = 16

NUM_TOKENS = GROUP_SIZE * TOKENS_DEV
NUM_PAIRS = NUM_TOKENS * TOP_K
BASE_LOAD = TOKENS_DEV * TOP_K // NUM_EXPERTS
CAPACITY = BASE_LOAD + BASE_LOAD // 2 + min(TOKENS_DEV * TOP_K % NUM_EXPERTS, 1)
EXPERT_ROWS = GROUP_SIZE * CAPACITY


def draw_routing(rng_key):
    perm_key, delta_key, tok_key, rot_key = jax.random.split(rng_key, 4)
    spread = BASE_LOAD // 2
    expert_range = jnp.arange(NUM_EXPERTS, dtype=jnp.int32)
    deltas = jax.random.randint(delta_key, (GROUP_SIZE, NUM_EXPERTS // 2), 0, spread + 1, dtype=jnp.int32)
    deltas = deltas.at[:, 0].set(spread)
    signed_delta = jnp.stack([deltas, -deltas], axis=-1).reshape(GROUP_SIZE, NUM_EXPERTS)
    extra_one = (expert_range < TOKENS_DEV * TOP_K % NUM_EXPERTS).astype(jnp.int32)
    dev_counts = BASE_LOAD + extra_one[None, :] + signed_delta
    labels = jax.random.permutation(perm_key, NUM_EXPERTS).astype(jnp.int32)
    pair_range = jnp.arange(TOKENS_DEV * TOP_K, dtype=jnp.int32)

    def one_device(counts, perm_seed, rot_seed):
        run_ends = jnp.cumsum(counts)
        sequence = jnp.searchsorted(run_ends, pair_range, side='right').astype(jnp.int32)
        slot_table = sequence.reshape(TOP_K, TOKENS_DEV).T
        slot_table = slot_table[jax.random.permutation(perm_seed, TOKENS_DEV)]
        rot_shift = jax.random.randint(rot_seed, (TOKENS_DEV, 1), 0, TOP_K, dtype=jnp.int32)
        col_order = (jnp.arange(TOP_K, dtype=jnp.int32)[None, :] + rot_shift) % TOP_K
        slot_table = jnp.take_along_axis(slot_table, col_order, axis=1)
        return labels[slot_table]

    routed_ids = jax.vmap(one_device)(dev_counts, jax.random.split(tok_key, GROUP_SIZE), jax.random.split(rot_key, GROUP_SIZE))
    return routed_ids.reshape(NUM_TOKENS, TOP_K)


def normal_weight(rng_key, shape, scale):
    return (jax.random.normal(rng_key, shape, jnp.float32) * scale).astype(jnp.bfloat16)


def setup_inputs(seed: int = 0, part: int = 0) -> dict:
    base_key = jax.random.key(seed)
    part_key = jax.random.fold_in(base_key, part)
    weight_keys = jax.random.split(base_key, 7)
    part_keys = jax.random.split(part_key, 2)
    in_scale = MODEL_DIM ** -0.5
    tokens = jax.random.normal(part_keys[0], (NUM_TOKENS, MODEL_DIM), jnp.float32).astype(jnp.bfloat16)
    return {
        'tokens': tokens,
        'w_router': normal_weight(weight_keys[0], (MODEL_DIM, NUM_EXPERTS), 2.0 * in_scale),
        'expert_ids': draw_routing(part_keys[1]),
        'w_gate': normal_weight(weight_keys[1], (NUM_EXPERTS, MODEL_DIM, EXPERT_FF), in_scale),
        'w_up': normal_weight(weight_keys[2], (NUM_EXPERTS, MODEL_DIM, EXPERT_FF), in_scale),
        'w_down': normal_weight(weight_keys[3], (NUM_EXPERTS, EXPERT_FF, MODEL_DIM), EXPERT_FF ** -0.5),
        'shared_gate': normal_weight(weight_keys[4], (MODEL_DIM, SHARED_FF), in_scale),
        'shared_up': normal_weight(weight_keys[5], (MODEL_DIM, SHARED_FF), in_scale),
        'shared_down': normal_weight(weight_keys[6], (SHARED_FF, MODEL_DIM), SHARED_FF ** -0.5),
    }


def swiglu(rows_in, w_one, w_three, w_two):
    gate_act = jnp.dot(rows_in, w_one, preferred_element_type=jnp.float32)
    up_act = jnp.dot(rows_in, w_three, preferred_element_type=jnp.float32)
    hidden = (jax.nn.silu(gate_act) * up_act).astype(jnp.bfloat16)
    return jnp.dot(hidden, w_two, preferred_element_type=jnp.float32).astype(jnp.bfloat16)


def reference(tokens, w_router, expert_ids, w_gate, w_up, w_down, shared_gate, shared_up, shared_down):
    logits = jnp.dot(tokens, w_router, preferred_element_type=jnp.float32)
    picked = jnp.take_along_axis(logits, expert_ids, axis=1)
    gate_vals = jax.nn.softmax(picked, axis=-1)
    flat_ids = expert_ids.reshape(-1)
    sort_order = jnp.argsort(flat_ids, stable=True)
    counts = jnp.bincount(flat_ids, length=NUM_EXPERTS)
    starts = jnp.cumsum(counts) - counts
    row_range = jnp.arange(EXPERT_ROWS)
    src_pos = jnp.minimum(starts[:, None] + row_range[None, :], NUM_PAIRS - 1)
    is_valid = row_range[None, :] < counts[:, None]
    pair_id = sort_order[src_pos]
    tok_table = jnp.where(is_valid, pair_id // TOP_K, NUM_TOKENS)
    gate_table = jnp.where(is_valid, gate_vals.reshape(-1)[pair_id], 0.0)
    shared_out = swiglu(tokens, shared_gate, shared_up, shared_down)

    def expert_step(running, step_in):
        rows_tok, rows_gate, w_one, w_three, w_two = step_in
        rows_in = jnp.take(tokens, rows_tok, axis=0, mode='fill', fill_value=0)
        out_rows = swiglu(rows_in, w_one, w_three, w_two)
        running = running.at[rows_tok].add(rows_gate[:, None] * out_rows.astype(jnp.float32), mode='drop')
        return running, None

    summed, unused_tail = lax.scan(expert_step, shared_out.astype(jnp.float32), (tok_table, gate_table, w_gate, w_up, w_down))
    return summed.astype(jnp.bfloat16)
```

```python
import functools

import jax
import jax.numpy as jnp
from jax import lax
from jax.experimental import pallas as pl
from jax.experimental.pallas import tpu as pltpu
from jax.sharding import PartitionSpec as P

MESH = pl.DeviceIdType.MESH
VMEM_LIMIT = 60 * 1024 * 1024


def capacity_of(tok_dev, top_k, num_exp):
    base_load = tok_dev * top_k // num_exp
    return base_load + base_load // 2 + min(tok_dev * top_k % num_exp, 1)


def gate_values(tok_rows, w_router, ids_loc):
    logits = jnp.dot(tok_rows, w_router, preferred_element_type=jnp.float32)
    expert_range = jnp.arange(w_router.shape[1], dtype=jnp.int32)
    hit = ids_loc[:, :, None] == expert_range[None, None, :]
    picked = jnp.sum(jnp.where(hit, logits[:, None, :], 0.0), axis=2)
    return jax.nn.softmax(picked, axis=-1)


def exchange_kernel(group, mine_ref, all_ref, send_sem, recv_sem):
    me = lax.axis_index('ep')
    barrier = pltpu.get_barrier_semaphore()
    for i in range(1, group):
        pl.semaphore_signal(barrier, inc=1, device_id={'ep': lax.rem(me + i, group)}, device_id_type=MESH)
    pl.semaphore_wait(barrier, group - 1)
    copies = []
    for i in range(1, group):
        copies.append(pltpu.make_async_remote_copy(
            src_ref=mine_ref,
            dst_ref=all_ref.at[me],
            send_sem=send_sem.at[i],
            recv_sem=recv_sem.at[i],
            device_id={'ep': lax.rem(me + i, group)},
            device_id_type=MESH,
        ))
    for copy in copies:
        copy.start()
    all_ref[pl.ds(me, 1)] = mine_ref[...][None]
    for copy in copies:
        copy.wait()


def exchange(mine, group):
    return pl.pallas_call(
        functools.partial(exchange_kernel, group),
        out_shape=jax.ShapeDtypeStruct((group,) + mine.shape, mine.dtype),
        in_specs=[pl.BlockSpec(memory_space=pltpu.VMEM)],
        out_specs=pl.BlockSpec(memory_space=pltpu.VMEM),
        scratch_shapes=[pltpu.SemaphoreType.DMA((group,)), pltpu.SemaphoreType.DMA((group,))],
        compiler_params=pltpu.CompilerParams(collective_id=0, has_side_effects=True),
    )(mine)


def dispatch_kernel(count, slots, *refs):
    chunks, rank_ref = refs[:count], refs[count]
    out_ref, buf, sem = refs[-3:]
    i = pl.program_id(0)
    num_loc, tok_dev = rank_ref.shape[1], rank_ref.shape[2]

    def fetch(k):
        return pltpu.make_async_copy(chunks[k], buf.at[k % 2], sem.at[k % 2])

    for k in range(count):
        @pl.when(i == k)
        def _(k=k):
            if k == 0:
                fetch(0).start()
            if k + 1 < count:
                fetch(k + 1).start()
            fetch(k).wait()
    slot_range = lax.broadcasted_iota(jnp.int32, (num_loc, slots, tok_dev), 1).astype(jnp.float32)
    chosen = rank_ref[0][:, None, :] == slot_range
    one_hot = jnp.where(chosen, 1.0, 0.0).reshape(num_loc * slots, tok_dev).astype(jnp.bfloat16)
    rows = jnp.dot(one_hot, buf[i % 2], preferred_element_type=jnp.float32)
    out_ref[...] = rows.astype(jnp.bfloat16).reshape(out_ref.shape)


def dispatch_rows(chunks, ranks, slots, first, total, so_far=None):
    count = len(chunks)
    tok_dev, width = chunks[0].shape
    num_loc = ranks.shape[1]
    flops = 2 * count * num_loc * slots * tok_dev * width
    kept = [] if so_far is None else [so_far]
    return pl.pallas_call(
        functools.partial(dispatch_kernel, count, slots),
        grid=(count,),
        out_shape=jax.ShapeDtypeStruct((num_loc, total * slots, width), jnp.bfloat16),
        in_specs=[pl.BlockSpec(memory_space=pl.ANY)] * count + [pl.BlockSpec((1, num_loc, tok_dev), lambda i: (i, 0, 0))] + [pl.BlockSpec(memory_space=pl.ANY)] * len(kept),
        out_specs=pl.BlockSpec((num_loc, slots, width), lambda i: (0, i + first, 0)),
        input_output_aliases={count + 1: 0} if kept else {},
        scratch_shapes=[pltpu.VMEM((2, tok_dev, width), jnp.bfloat16), pltpu.SemaphoreType.DMA((2,))],
        cost_estimate=pl.CostEstimate(flops=flops, bytes_accessed=4 * count * tok_dev * width, transcendentals=0),
        compiler_params=pltpu.CompilerParams(vmem_limit_bytes=VMEM_LIMIT),
    )(*chunks, ranks, *kept)


def expert_kernel(*refs):
    rows_ref, gate_ref, up_ref, down_ref = refs[:4]
    out_ref = refs[-1]
    rows = rows_ref[0]
    gate_act = jnp.dot(rows, gate_ref[0], preferred_element_type=jnp.float32)
    up_act = jnp.dot(rows, up_ref[0], preferred_element_type=jnp.float32)
    hidden = (jax.nn.silu(gate_act) * up_act).astype(jnp.bfloat16)
    out_ref[0] = jnp.dot(hidden, down_ref[0], preferred_element_type=jnp.float32).astype(jnp.bfloat16)


def expert_mlp(rows, w_gate, w_up, w_down, first, count, so_far=None):
    rows_per, width = rows.shape[1:]
    inner = w_gate.shape[2]
    kept = [] if so_far is None else [so_far]
    return pl.pallas_call(
        expert_kernel,
        grid=(count,),
        out_shape=jax.ShapeDtypeStruct(rows.shape, jnp.bfloat16),
        in_specs=[
            pl.BlockSpec((1, rows_per, width), lambda e: (e + first, 0, 0)),
            pl.BlockSpec((1, width, inner), lambda e: (e + first, 0, 0)),
            pl.BlockSpec((1, width, inner), lambda e: (e + first, 0, 0)),
            pl.BlockSpec((1, inner, width), lambda e: (e + first, 0, 0)),
        ] + [pl.BlockSpec(memory_space=pl.ANY)] * len(kept),
        out_specs=pl.BlockSpec((1, rows_per, width), lambda e: (e + first, 0, 0)),
        input_output_aliases={4: 0} if kept else {},
        cost_estimate=pl.CostEstimate(flops=6 * count * rows_per * width * inner, bytes_accessed=6 * count * width * inner, transcendentals=count * rows_per * inner),
        compiler_params=pltpu.CompilerParams(vmem_limit_bytes=VMEM_LIMIT),
    )(rows, w_gate, w_up, w_down, *kept)


def combine_kernel(sets, adds, *refs):
    row_refs, refs = refs[:sets], refs[sets:]
    rank_refs, refs = refs[:sets], refs[sets:]
    gate_refs, refs = refs[:sets], refs[sets:]
    add_refs, (out_ref, weights) = refs[:adds], refs[adds:]
    num_loc, slots = row_refs[0].shape[0], row_refs[0].shape[1]
    tok_dev = out_ref.shape[0]

    @pl.when(pl.program_id(0) == 0)
    def _():
        slot_range = lax.broadcasted_iota(jnp.int32, (num_loc, slots, tok_dev), 1).astype(jnp.float32)
        for s in range(sets):
            chosen = rank_refs[s][0][:, None, :] == slot_range
            gate = gate_refs[s][0]
            high = gate.astype(jnp.bfloat16).astype(jnp.float32)
            rest = gate - high
            middle = rest.astype(jnp.bfloat16).astype(jnp.float32)
            low = rest - middle
            for k, term in enumerate((high, middle, low)):
                value = jnp.where(chosen, term[:, None, :], 0.0).reshape(num_loc * slots, tok_dev)
                at = (3 * s + k) * num_loc * slots
                weights[at:at + num_loc * slots, :] = value.astype(jnp.bfloat16)

    total = None
    for add_ref in add_refs:
        value = add_ref[...].astype(jnp.float32)
        total = value if total is None else total + value
    rows = []
    for s in range(sets):
        rows += [row_refs[s][...].reshape(num_loc * slots, out_ref.shape[1])] * 3
    rows = jnp.concatenate(rows, axis=0)
    value = lax.dot_general(weights[...], rows, (((0,), (0,)), ((), ())), preferred_element_type=jnp.float32)
    total = value if total is None else total + value
    out_ref[...] = total.astype(out_ref.dtype)


def combine_rows(pieces, ranks, gates, slots, added, out_dtype=jnp.float32):
    num_loc, tok_dev = ranks.shape[1], ranks.shape[2]
    width = pieces[0][0].shape[2]
    cols = width // 2
    row_specs = [pl.BlockSpec((num_loc, slots, cols), lambda j, b=b: (0, b, j)) for _, b, _ in pieces]
    table_specs = [pl.BlockSpec((1, num_loc, tok_dev), lambda j, t=t: (t, 0, 0)) for _, _, t in pieces]
    flat_spec = pl.BlockSpec((tok_dev, cols), lambda j: (0, j))
    flops = 6 * len(pieces) * num_loc * slots * tok_dev * width
    return pl.pallas_call(
        functools.partial(combine_kernel, len(pieces), len(added)),
        grid=(2,),
        out_shape=jax.ShapeDtypeStruct((tok_dev, width), out_dtype),
        in_specs=row_specs + table_specs + table_specs + [flat_spec] * len(added),
        out_specs=flat_spec,
        scratch_shapes=[pltpu.VMEM((len(pieces) * 3 * num_loc * slots, tok_dev), jnp.bfloat16)],
        cost_estimate=pl.CostEstimate(flops=flops, bytes_accessed=4 * tok_dev * width * (1 + len(added)), transcendentals=0),
        compiler_params=pltpu.CompilerParams(vmem_limit_bytes=VMEM_LIMIT),
    )(*[p[0] for p in pieces], *[ranks] * len(pieces), *[gates] * len(pieces), *added)


def solution(mesh):
    group = mesh.shape['ep']
    ring = group // 2
    far = ring // 2
    row_spec = P(('dp', 'ep'), None)
    full_spec = P(None, None)
    expert_spec = P('ep', None, None)

    def index_of(z, core):
        return (z % ring) * 2 + core

    away_perm = [(index_of(z, c), index_of(z + (1 - 2 * c), c)) for z in range(ring) for c in range(2)]
    back_perm = [(dst, src) for src, dst in away_perm]
    swap_perm = [(i, i ^ 1) for i in range(group)]
    away_cross = [(src, dst ^ 1) for src, dst in away_perm]
    back_cross = [(src, dst ^ 1) for src, dst in back_perm]

    def away(value):
        return lax.ppermute(value, 'ep', away_perm)

    def back(value):
        return lax.ppermute(value, 'ep', back_perm)

    def swap(value):
        return lax.ppermute(value, 'ep', swap_perm)

    def device_step(tok_rows, w_router, ids_loc, w_gate, w_up, w_down, shared_gate, shared_up, shared_down):
        tok_dev, top_k = ids_loc.shape
        width = tok_rows.shape[1]
        num_exp = w_router.shape[1]
        num_loc = w_gate.shape[0]
        capacity = capacity_of(tok_dev, top_k, num_exp)
        slots = -(-capacity // 16) * 16
        me = lax.axis_index('ep')
        core = me % 2
        z = me // 2
        sign = 1 - 2 * core
        last = [ids_loc]

        def step(fn, *args):
            args, _ = lax.optimization_barrier((args, last[0]))
            out = fn(*args)
            last[0] = out
            return out

        def after(value, other):
            return lax.optimization_barrier((value, other))[0]

        def src(d, other):
            if other:
                return index_of(z + sign * d, 1 - core)
            return index_of(z - sign * d, core)

        def meta_of(rows, w_r, ids):
            gates = gate_values(rows, w_r, ids)
            return jnp.concatenate([ids.astype(jnp.float32).T, gates.T], axis=0).reshape(-1, 128)

        a_own = [tok_rows, away(tok_rows)]
        meta = step(meta_of, tok_rows, w_router, ids_loc)
        meta = step(lambda m: exchange(m, group), meta)
        a_own.append(away(after(a_own[1], meta)))

        def gate_act_of(rows, w_one):
            return jnp.dot(rows, w_one, preferred_element_type=jnp.float32)

        def hidden_of(rows, gate_act, w_three):
            up_act = jnp.dot(rows, w_three, preferred_element_type=jnp.float32)
            return (jax.nn.silu(gate_act) * up_act).astype(jnp.bfloat16)

        def down_of(hidden, w_two):
            return jnp.dot(hidden, w_two, preferred_element_type=jnp.float32).astype(jnp.bfloat16)

        pairs = {}
        sources, holders = [], []

        def need(name, source, holder):
            pairs[name] = len(sources)
            sources.append(source)
            holders.append(holder)

        for d in range(far + 1):
            need(('a', d, False), src(d, False), me)
            need(('a', d, True), src(d, True), me)
            need(('sa', d), src(d, False), index_of(z, 1 - core))
        for d in range(1, far):
            need(('b', d, False), src(-d, False), me)
            need(('b', d, True), src(-d, True), me)
            need(('sb', d), src(-d, False), index_of(z, 1 - core))
        for other in (False, True):
            held = core if not other else 1 - core
            need(('ra', other), src(far - 1, False), index_of(z + sign, held))
            need(('rb', other), src(-(far - 2), False), index_of(z - sign, held))

        def tables_of(m):
            picked = jnp.take(m.reshape(group, 2 * top_k, tok_dev), jnp.stack(sources), axis=0)
            ids = picked[:, None, :top_k, :].astype(jnp.int32)
            gates = picked[:, None, top_k:2 * top_k, :]
            experts = jnp.stack(holders)[:, None] * num_loc + jnp.arange(num_loc, dtype=jnp.int32)[None, :]
            hit = ids == experts[:, :, None, None]
            named = jnp.any(hit, axis=2)
            gate_of = jnp.sum(jnp.where(hit, gates, 0.0), axis=2)
            tok_range = jnp.arange(tok_dev)
            before = (tok_range[:, None] < tok_range[None, :]).astype(jnp.bfloat16)
            rank = jnp.einsum('net,tu->neu', named.astype(jnp.bfloat16), before, preferred_element_type=jnp.float32)
            return jnp.where(named, rank, -1.0), gate_of

        ranks, gates = step(tables_of, meta)
        half = num_loc // 2

        def mlp_first(rows):
            return step(lambda r, *w: expert_mlp(r, *w, 0, half), rows, w_gate, w_up, w_down)

        def mlp_rest(rows, so_far):
            return step(lambda r, s, *w: expert_mlp(r, *w, half, num_loc - half, s), rows, so_far, w_gate, w_up, w_down)

        def chunk_of(name):
            kind, d, other = name
            return {'a': (a_own, a_oth), 'b': (b_own, b_oth)}[kind][other][d]

        def gather_rows(names, start, stop, so_far=None):
            order = jnp.array([pairs[n] for n in names[start:stop]])
            chunks = [chunk_of(n) for n in names[start:stop]]
            return step(lambda c, r, s: dispatch_rows(c, r[order], slots, start, len(names), s), chunks, ranks, so_far)

        def blocks(out, start, stop):
            return step(lambda o: o[:, start * slots:stop * slots], out)

        def total(pieces, added=(), out_dtype=jnp.float32):
            def run(arrays, r, g, a):
                pieces_in = [(x, b, pairs[n]) for x, (_, b, n) in zip(arrays, pieces)]
                return combine_rows(pieces_in, r, g, slots, a, out_dtype)
            return step(run, [p[0] for p in pieces], ranks, gates, list(added))

        names_1 = [('a', far, False), ('a', far, True), ('a', 3, False), ('a', 2, False), ('a', 3, True), ('a', 2, True)]
        names_2 = [('a', 1, False), ('a', 0, False), ('a', 1, True), ('a', 0, True)]
        names_3 = [('b', 3, False), ('b', 3, True), ('b', 2, False), ('b', 1, False), ('b', 2, True), ('b', 1, True)]

        gate_act = step(gate_act_of, tok_rows, shared_gate)
        b_own, b_oth = [None], [None]
        a_oth = [swap(tok_rows), swap(a_own[1])]
        rows_2 = gather_rows(names_2, 0, 4)
        a_own.append(away(after(a_own[2], rows_2)))
        a_oth.append(swap(a_own[2]))
        out_2 = mlp_first(after(rows_2, a_own[2]))
        a_own.append(away(after(a_own[3], out_2)))
        a_oth.append(swap(a_own[3]))
        b_own.append(back(after(tok_rows, a_own[3])))
        out_2 = mlp_rest(after(rows_2, a_own[3]), out_2)
        oth_2 = swap(blocks(out_2, 2, 4))
        rows_1 = gather_rows(names_1, 2, 6)
        b_own.append(back(after(b_own[1], a_own[far])))
        b_own.append(back(b_own[2]))
        a_oth.append(swap(a_own[far]))
        b_oth += [swap(c) for c in b_own[1:]]

        rows_1 = gather_rows(names_1, 0, 2, rows_1)
        out_1 = mlp_first(rows_1)
        out_1 = mlp_rest(after(rows_1, b_own[2]), out_1)
        got_own = back(blocks(out_1, 0, 1))
        got_oth = lax.ppermute(blocks(out_1, 1, 2), 'ep', away_cross)
        oth_1 = swap(blocks(out_1, 4, 6))

        rows_3 = gather_rows(names_3, 0, 6)
        out_3 = mlp_first(rows_3)
        acc_a = back(total([(got_own, 0, ('ra', False)), (got_oth, 0, ('ra', True)), (out_1, 2, ('a', 3, False)), (oth_1, 0, ('sa', 3))]))
        out_3 = mlp_rest(rows_3, out_3)
        got_own = away(blocks(out_3, 0, 1))
        got_oth = lax.ppermute(blocks(out_3, 1, 2), 'ep', back_cross)
        oth_3 = swap(blocks(out_3, 4, 6))
        hidden = step(hidden_of, tok_rows, gate_act, shared_up)
        shared_out = step(down_of, hidden, shared_down)
        acc_a = back(total([(out_1, 3, ('a', 2, False)), (oth_1, 1, ('sa', 2))], [acc_a]))
        acc_b = away(total([(got_own, 0, ('rb', False)), (got_oth, 0, ('rb', True)), (out_3, 2, ('b', 2, False)), (oth_3, 0, ('sb', 2))]))
        acc_a = back(total([(out_2, 0, ('a', 1, False)), (oth_2, 0, ('sa', 1))], [acc_a]))
        acc_b = away(total([(out_3, 3, ('b', 1, False)), (oth_3, 1, ('sb', 1))], [acc_b]))
        return total([(out_2, 1, ('a', 0, False)), (oth_2, 1, ('sa', 0))], [shared_out, acc_a, acc_b], jnp.bfloat16)

    return jax.shard_map(device_step, mesh=mesh, in_specs=(row_spec, full_spec, row_spec, expert_spec, expert_spec, expert_spec, full_spec, full_spec, full_spec), out_specs=row_spec, check_vma=False)
```

```python
import functools

import jax
import jax.numpy as jnp
from jax import lax
from jax.experimental import pallas as pl
from jax.experimental.pallas import tpu as pltpu
from jax.sharding import PartitionSpec as P


MESH = pl.DeviceIdType.MESH
VMEM_LIMIT = 60 * 1024 * 1024


def capacity_of(tok_dev, top_k, num_exp):
    base_load = tok_dev * top_k // num_exp
    return base_load + base_load // 2 + min(tok_dev * top_k % num_exp, 1)


def gate_values(tok_rows, w_router, ids_loc):
    logits = jnp.dot(tok_rows, w_router, preferred_element_type=jnp.float32)
    expert_range = jnp.arange(w_router.shape[1], dtype=jnp.int32)
    hit = ids_loc[:, :, None] == expert_range[None, None, :]
    picked = jnp.sum(jnp.where(hit, logits[:, None, :], 0.0), axis=2)
    return jax.nn.softmax(picked, axis=-1)


def exchange_kernel(group, mine_ref, all_ref, send_sem, recv_sem):
    me = lax.axis_index('ep')
    barrier = pltpu.get_barrier_semaphore()
    for i in range(1, group):
        pl.semaphore_signal(barrier, inc=1, device_id={'ep': lax.rem(me + i, group)}, device_id_type=MESH)
    pl.semaphore_wait(barrier, group - 1)
    copies = []
    for i in range(1, group):
        copies.append(pltpu.make_async_remote_copy(
            src_ref=mine_ref,
            dst_ref=all_ref.at[me],
            send_sem=send_sem.at[i],
            recv_sem=recv_sem.at[i],
            device_id={'ep': lax.rem(me + i, group)},
            device_id_type=MESH,
        ))
    for copy in copies:
        copy.start()
    all_ref[pl.ds(me, 1)] = mine_ref[...][None]
    for copy in copies:
        copy.wait()


def exchange(mine, group):
    return pl.pallas_call(
        functools.partial(exchange_kernel, group),
        out_shape=jax.ShapeDtypeStruct((group,) + mine.shape, mine.dtype),
        in_specs=[pl.BlockSpec(memory_space=pltpu.VMEM)],
        out_specs=pl.BlockSpec(memory_space=pltpu.VMEM),
        scratch_shapes=[pltpu.SemaphoreType.DMA((group,)), pltpu.SemaphoreType.DMA((group,))],
        compiler_params=pltpu.CompilerParams(collective_id=0, has_side_effects=True),
    )(mine)


def dispatch_kernel(count, slots, *refs):
    chunks, rank_ref = refs[:count], refs[count]
    out_ref, buf, sem = refs[-3:]
    i = pl.program_id(0)
    num_loc, tok_dev = rank_ref.shape[1], rank_ref.shape[2]

    def fetch(k):
        return pltpu.make_async_copy(chunks[k], buf.at[k % 2], sem.at[k % 2])

    for k in range(count):
        @pl.when(i == k)
        def _(k=k):
            if k == 0:
                fetch(0).start()
            if k + 1 < count:
                fetch(k + 1).start()
            fetch(k).wait()
    slot_range = lax.broadcasted_iota(jnp.int32, (num_loc, slots, tok_dev), 1).astype(jnp.float32)
    chosen = rank_ref[0][:, None, :] == slot_range
    one_hot = jnp.where(chosen, 1.0, 0.0).reshape(num_loc * slots, tok_dev).astype(jnp.bfloat16)
    rows = jnp.dot(one_hot, buf[i % 2], preferred_element_type=jnp.float32)
    out_ref[...] = rows.astype(jnp.bfloat16).reshape(out_ref.shape)


def dispatch_rows(chunks, ranks, slots, first, total, so_far=None):
    count = len(chunks)
    tok_dev, width = chunks[0].shape
    num_loc = ranks.shape[1]
    flops = 2 * count * num_loc * slots * tok_dev * width
    kept = [] if so_far is None else [so_far]
    return pl.pallas_call(
        functools.partial(dispatch_kernel, count, slots),
        grid=(count,),
        out_shape=jax.ShapeDtypeStruct((num_loc, total * slots, width), jnp.bfloat16),
        in_specs=[pl.BlockSpec(memory_space=pl.ANY)] * count + [pl.BlockSpec((1, num_loc, tok_dev), lambda i: (i, 0, 0))] + [pl.BlockSpec(memory_space=pl.ANY)] * len(kept),
        out_specs=pl.BlockSpec((num_loc, slots, width), lambda i: (0, i + first, 0)),
        input_output_aliases={count + 1: 0} if kept else {},
        scratch_shapes=[pltpu.VMEM((2, tok_dev, width), jnp.bfloat16), pltpu.SemaphoreType.DMA((2,))],
        cost_estimate=pl.CostEstimate(flops=flops, bytes_accessed=4 * count * tok_dev * width, transcendentals=0),
        compiler_params=pltpu.CompilerParams(vmem_limit_bytes=VMEM_LIMIT),
    )(*chunks, ranks, *kept)


def expert_kernel(*refs):
    rows_ref, gate_ref, up_ref, down_ref = refs[:4]
    out_ref = refs[-1]
    rows = rows_ref[0]
    gate_act = jnp.dot(rows, gate_ref[0], preferred_element_type=jnp.float32)
    up_act = jnp.dot(rows, up_ref[0], preferred_element_type=jnp.float32)
    hidden = (jax.nn.silu(gate_act) * up_act).astype(jnp.bfloat16)
    out_ref[0] = jnp.dot(hidden, down_ref[0], preferred_element_type=jnp.float32).astype(jnp.bfloat16)


def expert_mlp(rows, w_gate, w_up, w_down, first, count, so_far=None):
    rows_per, width = rows.shape[1:]
    inner = w_gate.shape[2]
    kept = [] if so_far is None else [so_far]
    return pl.pallas_call(
        expert_kernel,
        grid=(count,),
        out_shape=jax.ShapeDtypeStruct(rows.shape, jnp.bfloat16),
        in_specs=[
            pl.BlockSpec((1, rows_per, width), lambda e: (e + first, 0, 0)),
            pl.BlockSpec((1, width, inner), lambda e: (e + first, 0, 0)),
            pl.BlockSpec((1, width, inner), lambda e: (e + first, 0, 0)),
            pl.BlockSpec((1, inner, width), lambda e: (e + first, 0, 0)),
        ] + [pl.BlockSpec(memory_space=pl.ANY)] * len(kept),
        out_specs=pl.BlockSpec((1, rows_per, width), lambda e: (e + first, 0, 0)),
        input_output_aliases={4: 0} if kept else {},
        cost_estimate=pl.CostEstimate(flops=6 * count * rows_per * width * inner, bytes_accessed=6 * count * width * inner, transcendentals=count * rows_per * inner),
        compiler_params=pltpu.CompilerParams(vmem_limit_bytes=VMEM_LIMIT),
    )(rows, w_gate, w_up, w_down, *kept)


def combine_kernel(sets, adds, *refs):
    row_refs, refs = refs[:sets], refs[sets:]
    rank_refs, refs = refs[:sets], refs[sets:]
    gate_refs, refs = refs[:sets], refs[sets:]
    add_refs, (out_ref, weights) = refs[:adds], refs[adds:]
    num_loc, slots = row_refs[0].shape[0], row_refs[0].shape[1]
    tok_dev = out_ref.shape[0]

    @pl.when(pl.program_id(0) == 0)
    def _():
        slot_range = lax.broadcasted_iota(jnp.int32, (num_loc, slots, tok_dev), 1).astype(jnp.float32)
        for s in range(sets):
            chosen = rank_refs[s][0][:, None, :] == slot_range
            gate = gate_refs[s][0]
            high = gate.astype(jnp.bfloat16).astype(jnp.float32)
            rest = gate - high
            middle = rest.astype(jnp.bfloat16).astype(jnp.float32)
            low = rest - middle
            for k, term in enumerate((high, middle, low)):
                value = jnp.where(chosen, term[:, None, :], 0.0).reshape(num_loc * slots, tok_dev)
                at = (3 * s + k) * num_loc * slots
                weights[at:at + num_loc * slots, :] = value.astype(jnp.bfloat16)

    total = None
    for add_ref in add_refs:
        value = add_ref[...].astype(jnp.float32)
        total = value if total is None else total + value
    rows = []
    for s in range(sets):
        rows += [row_refs[s][...].reshape(num_loc * slots, out_ref.shape[1])] * 3
    rows = jnp.concatenate(rows, axis=0)
    value = lax.dot_general(weights[...], rows, (((0,), (0,)), ((), ())), preferred_element_type=jnp.float32)
    total = value if total is None else total + value
    out_ref[...] = total.astype(out_ref.dtype)


def combine_rows(pieces, ranks, gates, slots, added, out_dtype=jnp.float32):
    num_loc, tok_dev = ranks.shape[1], ranks.shape[2]
    width = pieces[0][0].shape[2]
    cols = width // 2
    row_specs = [pl.BlockSpec((num_loc, slots, cols), lambda j, b=b: (0, b, j)) for _, b, _ in pieces]
    table_specs = [pl.BlockSpec((1, num_loc, tok_dev), lambda j, t=t: (t, 0, 0)) for _, _, t in pieces]
    flat_spec = pl.BlockSpec((tok_dev, cols), lambda j: (0, j))
    flops = 6 * len(pieces) * num_loc * slots * tok_dev * width
    return pl.pallas_call(
        functools.partial(combine_kernel, len(pieces), len(added)),
        grid=(2,),
        out_shape=jax.ShapeDtypeStruct((tok_dev, width), out_dtype),
        in_specs=row_specs + table_specs + table_specs + [flat_spec] * len(added),
        out_specs=flat_spec,
        scratch_shapes=[pltpu.VMEM((len(pieces) * 3 * num_loc * slots, tok_dev), jnp.bfloat16)],
        cost_estimate=pl.CostEstimate(flops=flops, bytes_accessed=4 * tok_dev * width * (1 + len(added)), transcendentals=0),
        compiler_params=pltpu.CompilerParams(vmem_limit_bytes=VMEM_LIMIT),
    )(*[p[0] for p in pieces], *[ranks] * len(pieces), *[gates] * len(pieces), *added)


def solution(mesh):
    group = mesh.shape['ep']
    ring = group // 2
    far = ring // 2
    row_spec = P(('dp', 'ep'), None)
    full_spec = P(None, None)
    expert_spec = P('ep', None, None)

    def index_of(z, core):
        return (z % ring) * 2 + core

    away_perm = [(index_of(z, c), index_of(z + (1 - 2 * c), c)) for z in range(ring) for c in range(2)]
    back_perm = [(dst, src) for src, dst in away_perm]
    swap_perm = [(i, i ^ 1) for i in range(group)]
    away_cross = [(src, dst ^ 1) for src, dst in away_perm]
    back_cross = [(src, dst ^ 1) for src, dst in back_perm]

    perms = {'away': away_perm, 'back': back_perm, 'swap': swap_perm, 'away_cross': away_cross, 'back_cross': back_cross}

    def send(way, value):
        return lax.ppermute(value, 'ep', perms[way])

    def device_step(tok_rows, w_router, ids_loc, w_gate, w_up, w_down, shared_gate, shared_up, shared_down):
        tok_dev, top_k = ids_loc.shape
        num_exp = w_router.shape[1]
        num_loc = w_gate.shape[0]
        capacity = capacity_of(tok_dev, top_k, num_exp)
        slots = -(-capacity // 16) * 16
        me = lax.axis_index('ep')
        core = me % 2
        z = me // 2
        sign = 1 - 2 * core
        last = [ids_loc]

        def step(fn, *args):
            args, _ = lax.optimization_barrier((args, last[0]))
            out = fn(*args)
            last[0] = out
            return out

        def after(value, other):
            return lax.optimization_barrier((value, other))[0]

        def src(d, other):
            if other:
                return index_of(z + sign * d, 1 - core)
            return index_of(z - sign * d, core)

        def meta_of(rows, w_r, ids):
            gates = gate_values(rows, w_r, ids)
            return jnp.concatenate([ids.astype(jnp.float32).T, gates.T], axis=0).reshape(-1, 128)

        def gate_act_of(rows, w_one):
            return jnp.dot(rows, w_one, preferred_element_type=jnp.float32)

        def hidden_of(rows, gate_act, w_three):
            up_act = jnp.dot(rows, w_three, preferred_element_type=jnp.float32)
            return (jax.nn.silu(gate_act) * up_act).astype(jnp.bfloat16)

        def down_of(hidden, w_two):
            return jnp.dot(hidden, w_two, preferred_element_type=jnp.float32).astype(jnp.bfloat16)

        pairs = {}
        sources, holders = [], []

        def need(name, source, holder):
            pairs[name] = len(sources)
            sources.append(source)
            holders.append(holder)

        for d in range(far + 1):
            need(('a', d, False), src(d, False), me)
            need(('a', d, True), src(d, True), me)
            need(('sa', d), src(d, False), index_of(z, 1 - core))
        for d in range(1, far):
            need(('b', d, False), src(-d, False), me)
            need(('b', d, True), src(-d, True), me)
            need(('sb', d), src(-d, False), index_of(z, 1 - core))
        for other in (False, True):
            held = core if not other else 1 - core
            need(('ra', other), src(far - 1, False), index_of(z + sign, held))
            need(('rb', other), src(-(far - 2), False), index_of(z - sign, held))

        def tables_of(m):
            picked = jnp.take(m.reshape(group, 2 * top_k, tok_dev), jnp.stack(sources), axis=0)
            ids = picked[:, None, :top_k, :].astype(jnp.int32)
            gates = picked[:, None, top_k:2 * top_k, :]
            experts = jnp.stack(holders)[:, None] * num_loc + jnp.arange(num_loc, dtype=jnp.int32)[None, :]
            hit = ids == experts[:, :, None, None]
            named = jnp.any(hit, axis=2)
            gate_of = jnp.sum(jnp.where(hit, gates, 0.0), axis=2)
            tok_range = jnp.arange(tok_dev)
            before = (tok_range[:, None] < tok_range[None, :]).astype(jnp.bfloat16)
            rank = jnp.einsum('net,tu->neu', named.astype(jnp.bfloat16), before, preferred_element_type=jnp.float32)
            return jnp.where(named, rank, -1.0), gate_of

        a_own, b_own = [tok_rows, send('away', tok_rows)], [None, send('back', tok_rows)]
        meta = step(meta_of, tok_rows, w_router, ids_loc)
        gate_act = step(gate_act_of, tok_rows, shared_gate)
        hidden = step(hidden_of, tok_rows, gate_act, shared_up)
        shared_out = step(down_of, hidden, shared_down)
        a_own.append(send('away', a_own[1]))
        meta = step(lambda m: exchange(m, group), meta)
        a_own.append(send('away', a_own[2]))
        ranks, gates = step(tables_of, meta)
        half = num_loc // 2

        def mlp_first(rows):
            return step(lambda r, *w: expert_mlp(r, *w, 0, half), rows, w_gate, w_up, w_down)

        def mlp_rest(rows, so_far):
            return step(lambda r, s, *w: expert_mlp(r, *w, half, num_loc - half, s), rows, so_far, w_gate, w_up, w_down)

        def chunk_of(name):
            kind, d, other = name
            return {'a': (a_own, a_oth), 'b': (b_own, b_oth)}[kind][other][d]

        def gather_rows(names, start, stop, so_far=None):
            order = jnp.array([pairs[n] for n in names[start:stop]])
            chunks = [chunk_of(n) for n in names[start:stop]]
            return step(lambda c, r, s: dispatch_rows(c, r[order], slots, start, len(names), s), chunks, ranks, so_far)

        def blocks(out, start, stop):
            return step(lambda o: o[:, start * slots:stop * slots], out)

        def total(pieces, added=(), out_dtype=jnp.float32):
            def run(arrays, r, g, a):
                pieces_in = [(x, b, pairs[n]) for x, (_, b, n) in zip(arrays, pieces)]
                return combine_rows(pieces_in, r, g, slots, a, out_dtype)

            return step(run, [p[0] for p in pieces], ranks, gates, list(added))

        names_0 = [('a', 2, False), ('a', 2, True)]
        names_1 = [('a', far, False), ('a', far, True), ('a', 3, False), ('a', 3, True)]
        names_2 = [('a', 1, False), ('a', 0, False), ('a', 1, True), ('a', 0, True)]
        names_3 = [('b', 3, False), ('b', 3, True), ('b', 2, False), ('b', 1, False), ('b', 2, True), ('b', 1, True)]

        a_oth = [send('swap', tok_rows)] + [send('swap', a_own[d]) for d in range(1, far)]
        b_oth = [None, send('swap', b_own[1])]
        rows_0 = gather_rows(names_0, 0, 2)
        out_0 = mlp_first(rows_0)
        a_own.append(send('away', a_own[3]))
        a_oth.append(send('swap', a_own[far]))
        out_0 = mlp_rest(rows_0, out_0)
        oth_0 = send('swap', blocks(out_0, 1, 2))
        rows_1 = gather_rows(names_1, 2, 4)
        b_own.append(send('back', after(b_own[1], a_own[far])))

        rows_1 = gather_rows(names_1, 0, 2, rows_1)
        out_1 = mlp_first(rows_1)
        b_own.append(send('back', b_own[2]))
        b_oth.append(send('swap', b_own[2]))
        out_1 = mlp_rest(rows_1, out_1)
        got_own = send('back', blocks(out_1, 0, 1))
        got_oth = send('away_cross', blocks(out_1, 1, 2))
        oth_1 = send('swap', blocks(out_1, 3, 4))
        b_oth.append(send('swap', b_own[3]))

        rows_3 = gather_rows(names_3, 0, 6)
        acc_a = send('back', total([(got_own, 0, ('ra', False)), (got_oth, 0, ('ra', True)), (out_1, 2, ('a', 3, False)), (oth_1, 0, ('sa', 3))]))
        out_3 = mlp_first(rows_3)
        out_3 = mlp_rest(rows_3, out_3)
        got_own = send('away', blocks(out_3, 0, 1))
        got_oth = send('back_cross', blocks(out_3, 1, 2))
        oth_3 = send('swap', blocks(out_3, 4, 6))
        acc_a = send('back', total([(out_0, 0, ('a', 2, False)), (oth_0, 0, ('sa', 2))], [acc_a]))
        rows_2 = gather_rows(names_2, 0, 4)
        out_2 = mlp_first(rows_2)
        acc_b = send('away', total([(got_own, 0, ('rb', False)), (got_oth, 0, ('rb', True)), (out_3, 2, ('b', 2, False)), (oth_3, 0, ('sb', 2))]))
        out_2 = mlp_rest(rows_2, out_2)
        oth_2 = send('swap', blocks(out_2, 2, 4))
        here = total([(out_2, 1, ('a', 0, False)), (oth_2, 1, ('sa', 0))], [shared_out])
        acc_a = send('back', total([(out_2, 0, ('a', 1, False)), (oth_2, 0, ('sa', 1))], [acc_a]))
        acc_b = send('away', total([(out_3, 3, ('b', 1, False)), (oth_3, 1, ('sb', 1))], [acc_b]))
        return step(lambda x, a, b: (x + a + b).astype(jnp.bfloat16), here, acc_a, acc_b)


    return jax.shard_map(device_step, mesh=mesh, in_specs=(row_spec, full_spec, row_spec, expert_spec, expert_spec, expert_spec, full_spec, full_spec, full_spec), out_specs=row_spec, check_vma=False)
```

```python
import functools

import jax
import jax.numpy as jnp
from jax import lax
from jax.experimental import pallas as pl
from jax.experimental.pallas import tpu as pltpu
from jax.sharding import PartitionSpec as P


MESH = pl.DeviceIdType.MESH
VMEM_LIMIT = 60 * 1024 * 1024


def capacity_of(tok_dev, top_k, num_exp):
    base_load = tok_dev * top_k // num_exp
    return base_load + base_load // 2 + min(tok_dev * top_k % num_exp, 1)


def gate_values(tok_rows, w_router, ids_loc):
    logits = jnp.dot(tok_rows, w_router, preferred_element_type=jnp.float32)
    expert_range = jnp.arange(w_router.shape[1], dtype=jnp.int32)
    hit = ids_loc[:, :, None] == expert_range[None, None, :]
    picked = jnp.sum(jnp.where(hit, logits[:, None, :], 0.0), axis=2)
    return jax.nn.softmax(picked, axis=-1)


def exchange_kernel(group, mine_ref, all_ref, send_sem, recv_sem):
    me = lax.axis_index('ep')
    barrier = pltpu.get_barrier_semaphore()
    for i in range(1, group):
        pl.semaphore_signal(barrier, inc=1, device_id={'ep': lax.rem(me + i, group)}, device_id_type=MESH)
    pl.semaphore_wait(barrier, group - 1)
    copies = []
    for i in range(1, group):
        copies.append(pltpu.make_async_remote_copy(
            src_ref=mine_ref,
            dst_ref=all_ref.at[me],
            send_sem=send_sem.at[i],
            recv_sem=recv_sem.at[i],
            device_id={'ep': lax.rem(me + i, group)},
            device_id_type=MESH,
        ))
    for copy in copies:
        copy.start()
    all_ref[pl.ds(me, 1)] = mine_ref[...][None]
    for copy in copies:
        copy.wait()


def exchange(mine, group):
    return pl.pallas_call(
        functools.partial(exchange_kernel, group),
        out_shape=jax.ShapeDtypeStruct((group,) + mine.shape, mine.dtype),
        in_specs=[pl.BlockSpec(memory_space=pltpu.VMEM)],
        out_specs=pl.BlockSpec(memory_space=pltpu.VMEM),
        scratch_shapes=[pltpu.SemaphoreType.DMA((group,)), pltpu.SemaphoreType.DMA((group,))],
        compiler_params=pltpu.CompilerParams(collective_id=0, has_side_effects=True),
    )(mine)


def dispatch_kernel(count, slots, *refs):
    chunks, rank_ref = refs[:count], refs[count]
    out_ref, buf, sem = refs[-3:]
    i = pl.program_id(0)
    num_loc, tok_dev = rank_ref.shape[1], rank_ref.shape[2]

    def fetch(k):
        return pltpu.make_async_copy(chunks[k], buf.at[k % 2], sem.at[k % 2])

    for k in range(count):
        @pl.when(i == k)
        def _(k=k):
            if k == 0:
                fetch(0).start()
            if k + 1 < count:
                fetch(k + 1).start()
            fetch(k).wait()
    slot_range = lax.broadcasted_iota(jnp.int32, (num_loc, slots, tok_dev), 1).astype(jnp.float32)
    chosen = rank_ref[0][:, None, :] == slot_range
    one_hot = jnp.where(chosen, 1.0, 0.0).reshape(num_loc * slots, tok_dev).astype(jnp.bfloat16)
    rows = jnp.dot(one_hot, buf[i % 2], preferred_element_type=jnp.float32)
    out_ref[...] = rows.astype(jnp.bfloat16).reshape(out_ref.shape)


def dispatch_rows(chunks, ranks, slots, first, total, so_far=None):
    count = len(chunks)
    tok_dev, width = chunks[0].shape
    num_loc = ranks.shape[1]
    flops = 2 * count * num_loc * slots * tok_dev * width
    kept = [] if so_far is None else [so_far]
    return pl.pallas_call(
        functools.partial(dispatch_kernel, count, slots),
        grid=(count,),
        out_shape=jax.ShapeDtypeStruct((num_loc, total * slots, width), jnp.bfloat16),
        in_specs=[pl.BlockSpec(memory_space=pl.ANY)] * count + [pl.BlockSpec((1, num_loc, tok_dev), lambda i: (i, 0, 0))] + [pl.BlockSpec(memory_space=pl.ANY)] * len(kept),
        out_specs=pl.BlockSpec((num_loc, slots, width), lambda i: (0, i + first, 0)),
        input_output_aliases={count + 1: 0} if kept else {},
        scratch_shapes=[pltpu.VMEM((2, tok_dev, width), jnp.bfloat16), pltpu.SemaphoreType.DMA((2,))],
        cost_estimate=pl.CostEstimate(flops=flops, bytes_accessed=4 * count * tok_dev * width, transcendentals=0),
        compiler_params=pltpu.CompilerParams(vmem_limit_bytes=VMEM_LIMIT),
    )(*chunks, ranks, *kept)


def expert_kernel(*refs):
    rows_ref, gate_ref, up_ref, down_ref = refs[:4]
    out_ref = refs[-1]
    rows = rows_ref[0]
    gate_act = jnp.dot(rows, gate_ref[0], preferred_element_type=jnp.float32)
    up_act = jnp.dot(rows, up_ref[0], preferred_element_type=jnp.float32)
    hidden = (jax.nn.silu(gate_act) * up_act).astype(jnp.bfloat16)
    out_ref[0] = jnp.dot(hidden, down_ref[0], preferred_element_type=jnp.float32).astype(jnp.bfloat16)


def expert_mlp(rows, w_gate, w_up, w_down, first, count, so_far=None):
    rows_per, width = rows.shape[1:]
    inner = w_gate.shape[2]
    kept = [] if so_far is None else [so_far]
    return pl.pallas_call(
        expert_kernel,
        grid=(count,),
        out_shape=jax.ShapeDtypeStruct(rows.shape, jnp.bfloat16),
        in_specs=[
            pl.BlockSpec((1, rows_per, width), lambda e: (e + first, 0, 0)),
            pl.BlockSpec((1, width, inner), lambda e: (e + first, 0, 0)),
            pl.BlockSpec((1, width, inner), lambda e: (e + first, 0, 0)),
            pl.BlockSpec((1, inner, width), lambda e: (e + first, 0, 0)),
        ] + [pl.BlockSpec(memory_space=pl.ANY)] * len(kept),
        out_specs=pl.BlockSpec((1, rows_per, width), lambda e: (e + first, 0, 0)),
        input_output_aliases={4: 0} if kept else {},
        cost_estimate=pl.CostEstimate(flops=6 * count * rows_per * width * inner, bytes_accessed=6 * count * width * inner, transcendentals=count * rows_per * inner),
        compiler_params=pltpu.CompilerParams(vmem_limit_bytes=VMEM_LIMIT),
    )(rows, w_gate, w_up, w_down, *kept)


def combine_kernel(sets, adds, *refs):
    row_refs, refs = refs[:sets], refs[sets:]
    rank_refs, refs = refs[:sets], refs[sets:]
    gate_refs, refs = refs[:sets], refs[sets:]
    add_refs, (out_ref, weights) = refs[:adds], refs[adds:]
    num_loc, slots = row_refs[0].shape[0], row_refs[0].shape[1]
    tok_dev = out_ref.shape[0]

    @pl.when(pl.program_id(0) == 0)
    def _():
        slot_range = lax.broadcasted_iota(jnp.int32, (num_loc, slots, tok_dev), 1).astype(jnp.float32)
        for s in range(sets):
            chosen = rank_refs[s][0][:, None, :] == slot_range
            gate = gate_refs[s][0]
            high = gate.astype(jnp.bfloat16).astype(jnp.float32)
            rest = gate - high
            middle = rest.astype(jnp.bfloat16).astype(jnp.float32)
            low = rest - middle
            for k, term in enumerate((high, middle, low)):
                value = jnp.where(chosen, term[:, None, :], 0.0).reshape(num_loc * slots, tok_dev)
                at = (3 * s + k) * num_loc * slots
                weights[at:at + num_loc * slots, :] = value.astype(jnp.bfloat16)

    total = None
    for add_ref in add_refs:
        value = add_ref[...].astype(jnp.float32)
        total = value if total is None else total + value
    rows = []
    for s in range(sets):
        rows += [row_refs[s][...].reshape(num_loc * slots, out_ref.shape[1])] * 3
    rows = jnp.concatenate(rows, axis=0)
    value = lax.dot_general(weights[...], rows, (((0,), (0,)), ((), ())), preferred_element_type=jnp.float32)
    total = value if total is None else total + value
    out_ref[...] = total.astype(out_ref.dtype)


def combine_rows(pieces, ranks, gates, slots, added, out_dtype=jnp.float32):
    num_loc, tok_dev = ranks.shape[1], ranks.shape[2]
    width = pieces[0][0].shape[2]
    cols = width // 2
    row_specs = [pl.BlockSpec((num_loc, slots, cols), lambda j, b=b: (0, b, j)) for _, b, _ in pieces]
    table_specs = [pl.BlockSpec((1, num_loc, tok_dev), lambda j, t=t: (t, 0, 0)) for _, _, t in pieces]
    flat_spec = pl.BlockSpec((tok_dev, cols), lambda j: (0, j))
    flops = 6 * len(pieces) * num_loc * slots * tok_dev * width
    return pl.pallas_call(
        functools.partial(combine_kernel, len(pieces), len(added)),
        grid=(2,),
        out_shape=jax.ShapeDtypeStruct((tok_dev, width), out_dtype),
        in_specs=row_specs + table_specs + table_specs + [flat_spec] * len(added),
        out_specs=flat_spec,
        scratch_shapes=[pltpu.VMEM((len(pieces) * 3 * num_loc * slots, tok_dev), jnp.bfloat16)],
        cost_estimate=pl.CostEstimate(flops=flops, bytes_accessed=4 * tok_dev * width * (1 + len(added)), transcendentals=0),
        compiler_params=pltpu.CompilerParams(vmem_limit_bytes=VMEM_LIMIT),
    )(*[p[0] for p in pieces], *[ranks] * len(pieces), *[gates] * len(pieces), *added)


def solution(mesh):
    group = mesh.shape['ep']
    ring = group // 2
    far = ring // 2
    row_spec = P(('dp', 'ep'), None)
    full_spec = P(None, None)
    expert_spec = P('ep', None, None)

    def index_of(z, core):
        return (z % ring) * 2 + core

    away_perm = [(index_of(z, c), index_of(z + (1 - 2 * c), c)) for z in range(ring) for c in range(2)]
    back_perm = [(dst, src) for src, dst in away_perm]
    swap_perm = [(i, i ^ 1) for i in range(group)]
    away_cross = [(src, dst ^ 1) for src, dst in away_perm]
    back_cross = [(src, dst ^ 1) for src, dst in back_perm]

    perms = {'away': away_perm, 'back': back_perm, 'swap': swap_perm, 'away_cross': away_cross, 'back_cross': back_cross}

    def send(way, value):
        return lax.ppermute(value, 'ep', perms[way])

    def device_step(tok_rows, w_router, ids_loc, w_gate, w_up, w_down, shared_gate, shared_up, shared_down):
        tok_dev, top_k = ids_loc.shape
        num_exp = w_router.shape[1]
        num_loc = w_gate.shape[0]
        capacity = capacity_of(tok_dev, top_k, num_exp)
        slots = -(-capacity // 16) * 16
        me = lax.axis_index('ep')
        core = me % 2
        z = me // 2
        sign = 1 - 2 * core
        last = [ids_loc]

        def step(fn, *args):
            args, _ = lax.optimization_barrier((args, last[0]))
            out = fn(*args)
            last[0] = out
            return out

        def after(value, other):
            return lax.optimization_barrier((value, other))[0]

        def src(d, other):
            if other:
                return index_of(z + sign * d, 1 - core)
            return index_of(z - sign * d, core)

        def meta_of(rows, w_r, ids):
            gates = gate_values(rows, w_r, ids)
            return jnp.concatenate([ids.astype(jnp.float32).T, gates.T], axis=0).reshape(-1, 128)

        def gate_act_of(rows, w_one):
            return jnp.dot(rows, w_one, preferred_element_type=jnp.float32)

        def hidden_of(rows, gate_act, w_three):
            up_act = jnp.dot(rows, w_three, preferred_element_type=jnp.float32)
            return (jax.nn.silu(gate_act) * up_act).astype(jnp.bfloat16)

        def down_of(hidden, w_two):
            return jnp.dot(hidden, w_two, preferred_element_type=jnp.float32).astype(jnp.bfloat16)

        pairs = {}
        sources, holders = [], []

        def need(name, source, holder):
            pairs[name] = len(sources)
            sources.append(source)
            holders.append(holder)

        for d in range(far + 1):
            need(('a', d, False), src(d, False), me)
            need(('a', d, True), src(d, True), me)
            need(('sa', d), src(d, False), index_of(z, 1 - core))
        for d in range(1, far):
            need(('b', d, False), src(-d, False), me)
            need(('b', d, True), src(-d, True), me)
            need(('sb', d), src(-d, False), index_of(z, 1 - core))
        for other in (False, True):
            held = core if not other else 1 - core
            need(('ra', other), src(far - 1, False), index_of(z + sign, held))
            need(('rb', other), src(-(far - 2), False), index_of(z - sign, held))

        def tables_of(m):
            picked = jnp.take(m.reshape(group, 2 * top_k, tok_dev), jnp.stack(sources), axis=0)
            ids = picked[:, None, :top_k, :].astype(jnp.int32)
            gates = picked[:, None, top_k:2 * top_k, :]
            experts = jnp.stack(holders)[:, None] * num_loc + jnp.arange(num_loc, dtype=jnp.int32)[None, :]
            hit = ids == experts[:, :, None, None]
            named = jnp.any(hit, axis=2)
            gate_of = jnp.sum(jnp.where(hit, gates, 0.0), axis=2)
            tok_range = jnp.arange(tok_dev)
            before = (tok_range[:, None] < tok_range[None, :]).astype(jnp.bfloat16)
            rank = jnp.einsum('net,tu->neu', named.astype(jnp.bfloat16), before, preferred_element_type=jnp.float32)
            return jnp.where(named, rank, -1.0), gate_of

        a_own, b_own = [tok_rows, send('away', tok_rows)], [None, send('back', tok_rows)]
        meta = step(meta_of, tok_rows, w_router, ids_loc)
        gate_act = step(gate_act_of, tok_rows, shared_gate)
        hidden = step(hidden_of, tok_rows, gate_act, shared_up)
        shared_out = step(down_of, hidden, shared_down)
        a_own.append(send('away', a_own[1]))
        meta = step(lambda m: exchange(m, group), meta)
        a_own.append(send('away', a_own[2]))
        ranks, gates = step(tables_of, meta)
        half = num_loc // 2

        def mlp_first(rows):
            return step(lambda r, *w: expert_mlp(r, *w, 0, half), rows, w_gate, w_up, w_down)

        def mlp_rest(rows, so_far):
            return step(lambda r, s, *w: expert_mlp(r, *w, half, num_loc - half, s), rows, so_far, w_gate, w_up, w_down)

        def chunk_of(name):
            kind, d, other = name
            return {'a': (a_own, a_oth), 'b': (b_own, b_oth)}[kind][other][d]

        def gather_rows(names, start, stop, so_far=None):
            order = jnp.array([pairs[n] for n in names[start:stop]])
            chunks = [chunk_of(n) for n in names[start:stop]]
            return step(lambda c, r, s: dispatch_rows(c, r[order], slots, start, len(names), s), chunks, ranks, so_far)

        def blocks(out, start, stop):
            return step(lambda o: o[:, start * slots:stop * slots], out)

        def total(pieces, added=(), out_dtype=jnp.float32):
            def run(arrays, r, g, a):
                pieces_in = [(x, b, pairs[n]) for x, (_, b, n) in zip(arrays, pieces)]
                return combine_rows(pieces_in, r, g, slots, a, out_dtype)

            return step(run, [p[0] for p in pieces], ranks, gates, list(added))

        names_0 = [('a', 2, False), ('a', 2, True)]
        names_1 = [('a', far, False), ('a', far, True), ('a', 3, False), ('a', 3, True)]
        names_2 = [('a', 1, False), ('a', 0, False), ('b', 1, False), ('a', 1, True), ('a', 0, True), ('b', 1, True)]
        names_3 = [('b', 3, False), ('b', 3, True), ('b', 2, False), ('b', 2, True)]

        a_oth = [send('swap', tok_rows)] + [send('swap', a_own[d]) for d in range(1, far)]
        b_oth = [None, send('swap', b_own[1])]
        rows_0 = gather_rows(names_0, 0, 2)
        out_0 = mlp_first(rows_0)
        a_own.append(send('away', a_own[3]))
        a_oth.append(send('swap', a_own[far]))
        out_0 = mlp_rest(rows_0, out_0)
        oth_0 = send('swap', blocks(out_0, 1, 2))
        rows_1 = gather_rows(names_1, 2, 4)
        b_own.append(send('back', after(b_own[1], a_own[far])))

        rows_1 = gather_rows(names_1, 0, 2, rows_1)
        out_1 = mlp_first(rows_1)
        b_own.append(send('back', b_own[2]))
        b_oth.append(send('swap', b_own[2]))
        out_1 = mlp_rest(rows_1, out_1)
        got_own = send('back', blocks(out_1, 0, 1))
        got_oth = send('away_cross', blocks(out_1, 1, 2))
        oth_1 = send('swap', blocks(out_1, 3, 4))
        b_oth.append(send('swap', b_own[3]))

        rows_3 = gather_rows(names_3, 0, 4)
        rows_2 = gather_rows(names_2, 0, 6)
        acc_a = send('back', total([(got_own, 0, ('ra', False)), (got_oth, 0, ('ra', True)), (out_1, 2, ('a', 3, False)), (oth_1, 0, ('sa', 3))]))
        out_3 = mlp_first(rows_3)
        out_3 = mlp_rest(rows_3, out_3)
        got_own = send('away', blocks(out_3, 0, 1))
        got_oth = send('back_cross', blocks(out_3, 1, 2))
        oth_3 = send('swap', blocks(out_3, 3, 4))
        acc_a = send('back', total([(out_0, 0, ('a', 2, False)), (oth_0, 0, ('sa', 2))], [acc_a]))
        out_2 = mlp_first(rows_2)
        acc_b = send('away', total([(got_own, 0, ('rb', False)), (got_oth, 0, ('rb', True)), (out_3, 2, ('b', 2, False)), (oth_3, 0, ('sb', 2))]))
        out_2 = mlp_rest(rows_2, out_2)
        oth_2 = send('swap', blocks(out_2, 3, 6))
        acc_a = send('back', total([(out_2, 0, ('a', 1, False)), (oth_2, 0, ('sa', 1))], [acc_a]))
        acc_b = send('away', total([(out_2, 2, ('b', 1, False)), (oth_2, 2, ('sb', 1))], [acc_b]))
        here = total([(out_2, 1, ('a', 0, False)), (oth_2, 1, ('sa', 0))], [shared_out])
        return step(lambda x, a, b: (x + a + b).astype(jnp.bfloat16), here, acc_a, acc_b)


    return jax.shard_map(device_step, mesh=mesh, in_specs=(row_spec, full_spec, row_spec, expert_spec, expert_spec, expert_spec, full_spec, full_spec, full_spec), out_specs=row_spec, check_vma=False)
```
